32 devices in a mesh: dp: 2 (over core), tensor: 16 (over z, y, x).
Axes of the slice: x: 2, y: 2, z: 4, core: 2. Of those that a mesh axis runs over, the one named last changes fastest.
Arguments:
- resid_stream: bfloat16 [512, 4608], P(('dp', 'tensor')), parts along dimension 0, may hold values from -120 to 120, as said below
- pre_gain: float32 [4608], replicated, may hold values from 0.5 to 1.5
- w_gate: bfloat16 [4608, 6144], P(None, 'tensor'), may hold values from -0.09375 to 0.09375
- w_up: bfloat16 [4608, 6144], P(None, 'tensor'), may hold values from -0.09375 to 0.09375
- w_down: bfloat16 [6144, 4608], P('tensor'), may hold values from -0.078125 to 0.078125
- post_gain: float32 [4608], replicated, may hold values from 0.5 to 1.5
Outputs:
- resid_out: bfloat16 [512, 4608], P(('dp', 'tensor')), parts along dimension 0
The draws below stay inside these ranges and needn't reach their ends.
There are 2 independent parts, one for each index of `dp`. The reference program is written for one: setup_inputs(seed, part) draws one part's arguments, and reference() takes and returns one part's arrays. A program takes and returns all parts, laid end to end along the dimension named above; an argument that names none is the same for every part. Nothing has to cross between parts.
Inputs may be any that keep to these rules, and one draw needn't show every extreme that they name: `resid_stream`: entries are real-valued.
All inputs are finite; a program needn't handle non-finite values.
Results may differ from the reference program's by a relative error of at most 0.0029.
Values may be sent and summed in bfloat16 or wider, within the bound.
A program may use at most 128 MiB of HBM per device.

```python
import jax
import jax.numpy as jnp
from jax import lax

D = 4608
TOKENS = 256
FF_WIN = 6144


def draw_resid_stream(key, part):
    keys = jax.random.split(jax.random.fold_in(key, 17), 3)
    base = jnp.clip(jax.random.normal(keys[0], (TOKENS, D), jnp.float32), -4.0, 4.0)
    row_scale = jnp.exp(jax.random.uniform(keys[1], (TOKENS, 1), jnp.float32) * 2.302585)
    col_scale = jnp.exp(jax.random.uniform(keys[2], (1, D), jnp.float32, minval=-1.15, maxval=1.15))
    values = base * row_scale * col_scale
    return jnp.clip(values, -120.0, 120.0).astype(jnp.bfloat16)


def level_of(rng, shape, pieces, low, high):
    level = 1.0
    for position, shards_of in pieces:
        draws = jax.random.uniform(jax.random.fold_in(jax.random.fold_in(rng, 6), position), (shards_of,), jnp.float32, low / len(pieces), high / len(pieces))
        level = level * jnp.repeat(jnp.exp(draws), shape[position] // shards_of).reshape((-1,) + (1,) * (len(shape) - 1 - position))
    return level


def bell_draw(key, dims, scale, limit, pieces=(), kind=jnp.bfloat16):
    result = jax.random.normal(key, dims, jnp.float32) * scale
    if len(pieces) > 0:
        result = level_of(key, dims, pieces, -0.22, 0.18) * result
    return jnp.clip(result, min=-limit, max=limit).astype(kind)


def setup_inputs(seed: int = 0, part: int = 0) -> dict:
    key_list = jax.random.split(jax.random.key(seed), 7)
    part_keys = jax.random.split(jax.random.fold_in(key_list[6], part), 7)
    resid_stream = draw_resid_stream(jax.random.fold_in(jax.random.fold_in(key_list[6], part), 71), part)
    pre_gain = jnp.clip(1.0 + 0.1 * jax.random.normal(key_list[1], (D,), jnp.float32), 0.5, 1.5)
    w_gate = bell_draw(key_list[2], (D, FF_WIN), D ** -0.5, 0.09375, ((1, 16),))
    w_up = bell_draw(key_list[3], (D, FF_WIN), D ** -0.5, 0.09375, ((1, 16),))
    w_down = bell_draw(key_list[4], (FF_WIN, D), FF_WIN ** -0.5, 0.078125, ((0, 16),))
    post_gain = jnp.clip(1.0 + 0.1 * jax.random.normal(key_list[5], (D,), jnp.float32), 0.5, 1.5)
    return {"resid_stream": resid_stream, "pre_gain": pre_gain, "w_gate": w_gate, "w_up": w_up, "w_down": w_down, "post_gain": post_gain}


norm_eps = 1e-06

def rms_scale(values):
    return values * lax.rsqrt(lax.optimization_barrier(jnp.mean(values * values, axis=-1, keepdims=True)) + norm_eps)

def reference(resid_stream, pre_gain, w_gate, w_up, w_down, post_gain):
    stream = resid_stream.astype(jnp.float32)
    normed = (rms_scale(stream) * pre_gain.astype(jnp.float32)).astype(jnp.bfloat16)
    gate_out = jnp.dot(normed, w_gate, preferred_element_type=jnp.float32)
    up_out = jnp.dot(normed, w_up, preferred_element_type=jnp.float32)
    hidden = (jax.nn.gelu(gate_out, approximate=True) * up_out).astype(jnp.bfloat16)
    block_out = jnp.dot(hidden, w_down, preferred_element_type=jnp.float32)
    post = (rms_scale(block_out) * post_gain.astype(jnp.float32)).astype(jnp.bfloat16)
    post = lax.optimization_barrier(post)
    return (stream + post.astype(jnp.float32)).astype(jnp.bfloat16)
```

```python
import functools

import jax
import jax.numpy as jnp
from jax import lax
from jax.experimental import pallas as pl
from jax.experimental.pallas import tpu as pltpu
from jax.sharding import PartitionSpec as P

norm_eps = 1e-06
SIDE = 2
PLANE = SIDE * SIDE
LINE = 4
MESH = pl.DeviceIdType.MESH


def shards(resid_stream, pre_gain, w_gate, w_up, w_down, post_gain):
    stream = resid_stream.astype(jnp.float32)
    local_norm = stream * lax.rsqrt(jnp.mean(stream * stream, axis=1, keepdims=True) + norm_eps)
    normed = (local_norm * pre_gain).astype(jnp.bfloat16)
    row_piece = lax.all_gather(normed, "tensor", axis=0, tiled=True)
    gate_out = jnp.dot(row_piece, w_gate, preferred_element_type=jnp.float32)
    up_out = jnp.dot(row_piece, w_up, preferred_element_type=jnp.float32)
    hidden = (jax.nn.gelu(gate_out, approximate=True) * up_out).astype(jnp.bfloat16)
    block_rows = lax.psum_scatter(
        jnp.dot(hidden, w_down, preferred_element_type=jnp.float32),
        "tensor",
        scatter_dimension=0,
        tiled=True,
    )
    row_factor = lax.rsqrt(jnp.mean(block_rows * block_rows, axis=1, keepdims=True) + norm_eps)
    post = (block_rows * row_factor * post_gain).astype(jnp.bfloat16)
    post = lax.optimization_barrier(post)
    return (stream + post.astype(jnp.float32)).astype(jnp.bfloat16)


def tile_of(size, most):
    return max(t for t in range(128, most + 1, 128) if size % t == 0)


def kernel(
    stream_ref, pre_ref, wg_hbm, wu_hbm, wd_hbm, post_ref, out_ref,
    w1, w2, gath, gu, hid, part, sendb, rda, rdb, xr, yr, zr,
    wsem, ssem, agz, agx, agy, agd, rsd, rsx, rsy, rsz,
):
    rows, d = stream_ref.shape
    ff = wg_hbm.shape[1]
    half = d // 2
    group = PLANE * rows
    A, B = pl.ds(0, half), pl.ds(half, half)

    loads = [
        pltpu.make_async_copy(wg_hbm, w1.at[:, pl.ds(0, ff)], wsem.at[0]),
        pltpu.make_async_copy(wu_hbm, w1.at[:, pl.ds(ff, ff)], wsem.at[1]),
        pltpu.make_async_copy(wd_hbm, w2, wsem.at[2]),
    ]
    for load in loads:
        load.start()

    me = lax.axis_index("tensor")
    x = lax.rem(me, SIDE)
    y = lax.rem(lax.div(me, SIDE), SIDE)
    z = lax.div(me, PLANE)
    spot = lax.rem(me, PLANE)
    sx = 1 - 2 * x
    sy = SIDE * (1 - 2 * y)
    xn, yn = me + sx, me + sy
    flip = lax.div(z, LINE // 2)
    p = z + flip * (LINE - 1 - 2 * z)
    inner = p == 1
    far = me + PLANE * (1 - 2 * flip)
    near = me - PLANE * (1 - 2 * flip)

    def plane_of(v):
        return v + flip * (LINE - 1 - 2 * v)

    order = [plane_of(p), plane_of(1 - p), plane_of(2), plane_of(3)]

    def blk(s, shift):
        return pl.ds(pl.multiple_of((s * PLANE + spot + shift) * rows, rows), rows)

    pending = []

    def send(src, dst, recv_sem, target, cond=None):
        copy = pltpu.make_async_remote_copy(
            src_ref=src, dst_ref=dst, send_sem=ssem.at[len(pending)], recv_sem=recv_sem,
            device_id={"tensor": target}, device_id_type=MESH,
        )
        pending.append((copy, cond))
        if cond is None:
            copy.start()
        else:
            pl.when(cond)(copy.start)

    def arrive(dst, recv_sem):
        pltpu.make_async_remote_copy(
            src_ref=dst, dst_ref=dst, send_sem=ssem.at[0], recv_sem=recv_sem,
            device_id={"tensor": xn}, device_id_type=MESH,
        ).wait_recv()

    barrier = pltpu.get_barrier_semaphore()
    for other in (xn, yn, far):
        pl.semaphore_signal(barrier, inc=1, device_id={"tensor": other}, device_id_type=MESH)

    @pl.when(inner)
    def _():
        pl.semaphore_signal(barrier, inc=1, device_id={"tensor": near}, device_id_type=MESH)

    stream = stream_ref[...].astype(jnp.float32)
    scale = lax.rsqrt(jnp.mean(stream * stream, axis=1, keepdims=True) + norm_eps)
    gath[blk(z, 0), :] = (stream * scale * pre_ref[...]).astype(jnp.bfloat16)

    pl.semaphore_wait(barrier, 3 + p)

    def along(k):
        s = order[k]
        ref = gath.at[blk(s, 0)]
        if k > 0:
            arrive(ref, agz.at[s])
        if k == 0:
            send(ref, ref, agz.at[s], far)
        if k == 1:
            send(ref, ref, agz.at[s], far, inner)
        else:
            send(ref, ref, agz.at[s], near, inner)
        for cols, kind in ((A, 0), (B, 1)):
            ref = gath.at[blk(s, 0), cols]
            send(ref, ref, agx.at[kind, s], xn)
            other = B if kind == 0 else A
            ref = gath.at[blk(s, 0), other]
            send(ref, ref, agy.at[1 - kind, s], yn)

    def across(k):
        s = order[k]
        ref = gath.at[blk(s, sx), A]
        arrive(ref, agx.at[0, s])
        send(ref, ref, agd.at[0, s], yn)
        ref = gath.at[blk(s, sy), B]
        arrive(ref, agy.at[1, s])
        send(ref, ref, agd.at[1, s], xn)

    tile = tile_of(2 * ff, 256)

    def first_dots(k):
        s = order[k]
        arrive(gath.at[blk(s, sx), B], agx.at[1, s])
        arrive(gath.at[blk(s, sy), A], agy.at[0, s])
        arrive(gath.at[blk(s, sx + sy), A], agd.at[0, s])
        arrive(gath.at[blk(s, sx + sy), B], agd.at[1, s])
        if k == 0:
            loads[0].wait()
            loads[1].wait()
        at = pl.ds(pl.multiple_of(s * group, group), group)

        @pl.loop(0, 2 * ff // tile)
        def _(i):
            cols = pl.ds(pl.multiple_of(i * tile, tile), tile)
            gu[:, cols] = jnp.dot(gath[at, :], w1[:, cols], preferred_element_type=jnp.float32)

        gate, up = gu[:, :ff], gu[:, ff:]
        hid[at, :] = (jax.nn.gelu(gate, approximate=True) * up).astype(jnp.bfloat16)

    along(0)
    across(0)
    along(1)
    first_dots(0)
    across(1)
    along(2)
    first_dots(1)
    across(2)
    along(3)
    first_dots(2)
    across(3)
    first_dots(3)

    back = order[::-1]
    wide = tile_of(half, 768)

    def last_dot(j):
        s = back[j]
        if j == 0:
            loads[2].wait()
        at = pl.ds(pl.multiple_of(s * group, group), group)

        @pl.loop(0, d // wide)
        def _(i):
            cols = pl.ds(pl.multiple_of(i * wide, wide), wide)
            res = jnp.dot(hid[at, :], w2[:, cols], preferred_element_type=jnp.float32)
            part[at, cols] = res
            sendb[at, cols] = res.astype(jnp.bfloat16)

        send(sendb.at[blk(s, sx + sy), A], rda.at[s], rsd.at[0, s], xn)
        send(sendb.at[blk(s, sx + sy), B], rdb.at[s], rsd.at[1, s], yn)
        send(sendb.at[blk(s, sx), A], xr.at[s, :, A], rsx.at[0, s], xn)
        send(sendb.at[blk(s, sy), B], yr.at[s, :, B], rsy.at[1, s], yn)

    def pass_on(j):
        s = back[j]
        arrive(rda.at[s], rsd.at[0, s])
        at = blk(s, sy)
        sendb[at, A] = (part[at, A] + rda[s].astype(jnp.float32)).astype(jnp.bfloat16)
        send(sendb.at[at, A], yr.at[s, :, A], rsy.at[0, s], yn)
        arrive(rdb.at[s], rsd.at[1, s])
        at = blk(s, sx)
        sendb[at, B] = (part[at, B] + rdb[s].astype(jnp.float32)).astype(jnp.bfloat16)
        send(sendb.at[at, B], xr.at[s, :, B], rsx.at[1, s], xn)

    def settle(j):
        s = back[j]
        arrive(xr.at[s, :, A], rsx.at[0, s])
        arrive(yr.at[s, :, B], rsy.at[1, s])
        arrive(yr.at[s, :, A], rsy.at[0, s])
        arrive(xr.at[s, :, B], rsx.at[1, s])
        at = blk(s, 0)
        part[at, :] += xr[s].astype(jnp.float32) + yr[s].astype(jnp.float32)

        def add(way):
            arrive(zr.at[way, s], rsz.at[way, s])
            part[at, :] += zr[way, s].astype(jnp.float32)

        outward, inward = flip, 1 - flip
        if j == LINE - 1:
            add(inward)
        pl.when(inner)(lambda: add(inward if j == LINE - 2 else outward))
        if j < LINE - 1:
            sendb[at, :] = part[at, :].astype(jnp.bfloat16)
            turn = p if j == LINE - 2 else 0
            way = flip + turn * (1 - 2 * flip)
            target = far + turn * (near - far)
            send(sendb.at[at], zr.at[way, s], rsz.at[way, s], target)

    last_dot(0)
    last_dot(1)
    pass_on(0)
    last_dot(2)
    pass_on(1)
    settle(0)
    last_dot(3)
    pass_on(2)
    settle(1)
    pass_on(3)
    settle(2)
    settle(3)

    total = part[blk(z, 0), :]
    factor = lax.rsqrt(jnp.mean(total * total, axis=1, keepdims=True) + norm_eps)
    post = (total * factor * post_ref[...]).astype(jnp.bfloat16)
    stream = stream_ref[...].astype(jnp.float32)
    out_ref[...] = (stream + post.astype(jnp.float32)).astype(jnp.bfloat16)

    for copy, cond in pending:
        if cond is None:
            copy.wait_send()
        else:
            pl.when(cond)(copy.wait_send)


def fused(resid_stream, pre_gain, w_gate, w_up, w_down, post_gain):
    rows, d = resid_stream.shape
    ff = w_gate.shape[1]
    n = PLANE * LINE
    bf, f32, dma = jnp.bfloat16, jnp.float32, pltpu.SemaphoreType.DMA
    vmem = pl.BlockSpec(memory_space=pltpu.VMEM)
    hbm = pl.BlockSpec(memory_space=pl.ANY)
    return pl.pallas_call(
        kernel,
        out_shape=jax.ShapeDtypeStruct((rows, d), bf),
        in_specs=[vmem, vmem, hbm, hbm, hbm, vmem],
        out_specs=vmem,
        scratch_shapes=[
            pltpu.VMEM((d, 2 * ff), bf),
            pltpu.VMEM((ff, d), bf),
            pltpu.VMEM((n * rows, d), bf),
            pltpu.VMEM((PLANE * rows, 2 * ff), f32),
            pltpu.VMEM((n * rows, ff), bf),
            pltpu.VMEM((n * rows, d), f32),
            pltpu.VMEM((n * rows, d), bf),
            pltpu.VMEM((LINE, rows, d // 2), bf),
            pltpu.VMEM((LINE, rows, d // 2), bf),
            pltpu.VMEM((LINE, rows, d), bf),
            pltpu.VMEM((LINE, rows, d), bf),
            pltpu.VMEM((2, LINE, rows, d), bf),
            dma((3,)),
            dma((80,)),
            dma((LINE,)),
            dma((2, LINE)),
            dma((2, LINE)),
            dma((2, LINE)),
            dma((2, LINE)),
            dma((2, LINE)),
            dma((2, LINE)),
            dma((2, LINE)),
        ],
        compiler_params=pltpu.CompilerParams(
            collective_id=0, has_side_effects=True, vmem_limit_bytes=60 * 2**20
        ),
        name="ffn",
    )(resid_stream, pre_gain.reshape(1, d), w_gate, w_up, w_down, post_gain.reshape(1, d))


def solution(mesh):
    body = fused if mesh.shape["tensor"] == PLANE * LINE else shards
    return jax.shard_map(
        body,
        mesh=mesh,
        in_specs=(
            P(("dp", "tensor"), None),
            P(),
            P(None, "tensor"),
            P(None, "tensor"),
            P("tensor", None),
            P(),
        ),
        out_specs=P(("dp", "tensor"), None),
        check_vma=False,
    )
```

```python
import functools

import jax
import jax.numpy as jnp
from jax import lax
from jax.experimental import pallas as pl
from jax.experimental.pallas import tpu as pltpu
from jax.sharding import PartitionSpec as P

norm_eps = 1e-06
SIDE = 2
PLANE = SIDE * SIDE
LINE = 4
MESH = pl.DeviceIdType.MESH


def shards(resid_stream, pre_gain, w_gate, w_up, w_down, post_gain):
    stream = resid_stream.astype(jnp.float32)
    local_norm = stream * lax.rsqrt(jnp.mean(stream * stream, axis=1, keepdims=True) + norm_eps)
    normed = (local_norm * pre_gain).astype(jnp.bfloat16)
    row_piece = lax.all_gather(normed, "tensor", axis=0, tiled=True)
    gate_out = jnp.dot(row_piece, w_gate, preferred_element_type=jnp.float32)
    up_out = jnp.dot(row_piece, w_up, preferred_element_type=jnp.float32)
    hidden = (jax.nn.gelu(gate_out, approximate=True) * up_out).astype(jnp.bfloat16)
    block_rows = lax.psum_scatter(
        jnp.dot(hidden, w_down, preferred_element_type=jnp.float32),
        "tensor",
        scatter_dimension=0,
        tiled=True,
    )
    row_factor = lax.rsqrt(jnp.mean(block_rows * block_rows, axis=1, keepdims=True) + norm_eps)
    post = (block_rows * row_factor * post_gain).astype(jnp.bfloat16)
    post = lax.optimization_barrier(post)
    return (stream + post.astype(jnp.float32)).astype(jnp.bfloat16)


def tile_of(size, most):
    return max(t for t in range(128, most + 1, 128) if size % t == 0)


def kernel(
    stream_ref, pre_ref, wg_hbm, wu_hbm, wd_hbm, post_ref, out_ref,
    w1, w2, gath, gu, hid, part, sendb, rda, rdb, xr, yr, zr,
    wsem, ssem, agz, agx, agy, agd, rsd, rsx, rsy, rsz,
):
    rows, d = stream_ref.shape
    ff = wg_hbm.shape[1]
    half = d // 2
    group = PLANE * rows
    A, B = halves = pl.ds(0, half), pl.ds(half, half)

    me = lax.axis_index("tensor")
    x = lax.rem(me, SIDE)
    y = lax.rem(lax.div(me, SIDE), SIDE)
    z = lax.div(me, PLANE)
    spot = lax.rem(me, PLANE)
    sx = 1 - 2 * x
    sy = SIDE * (1 - 2 * y)
    xn, yn = me + sx, me + sy
    flip = lax.div(z, LINE // 2)
    p = z + flip * (LINE - 1 - 2 * z)
    inner, outer = p == 1, p == 0
    far = me + PLANE * (1 - 2 * flip)
    near = me - PLANE * (1 - 2 * flip)

    barrier = pltpu.get_barrier_semaphore()
    for other in (xn, yn, far):
        pl.semaphore_signal(barrier, inc=1, device_id={"tensor": other}, device_id_type=MESH)

    @pl.when(inner)
    def _():
        pl.semaphore_signal(barrier, inc=1, device_id={"tensor": near}, device_id_type=MESH)

    loads = [
        pltpu.make_async_copy(wg_hbm, w1.at[:, pl.ds(0, ff)], wsem.at[0]),
        pltpu.make_async_copy(wu_hbm, w1.at[:, pl.ds(ff, ff)], wsem.at[1]),
        pltpu.make_async_copy(wd_hbm, w2, wsem.at[2]),
    ]
    for load in loads:
        load.start()

    def plane_of(v):
        return v + flip * (LINE - 1 - 2 * v)

    order = [plane_of(p), plane_of(1 - p), plane_of(2), plane_of(3)]

    def blk(s, shift):
        return pl.ds(pl.multiple_of((s * PLANE + spot + shift) * rows, rows), rows)

    pending = []

    def send(src, dst, recv_sem, target, cond=None, inside=False):
        copy = pltpu.make_async_remote_copy(
            src_ref=src, dst_ref=dst, send_sem=ssem.at[len(pending)], recv_sem=recv_sem,
            device_id={"tensor": target}, device_id_type=MESH,
        )
        pending.append(cond)
        if cond is None or inside:
            copy.start()
        else:
            pl.when(cond)(copy.start)

    def arrive(dst, recv_sem):
        pltpu.make_async_remote_copy(
            src_ref=dst, dst_ref=dst, send_sem=ssem.at[0], recv_sem=recv_sem,
            device_id={"tensor": xn}, device_id_type=MESH,
        ).wait_recv()

    stream = stream_ref[...].astype(jnp.float32)
    scale = lax.rsqrt(jnp.mean(stream * stream, axis=1, keepdims=True) + norm_eps)
    gath[blk(z, 0), :] = (stream * scale * pre_ref[...][None]).astype(jnp.bfloat16)

    pl.semaphore_wait(barrier, 3 + p)

    def along(k, kind):
        s = order[k]
        ref = gath.at[blk(s, 0), halves[kind]]
        if k > 0:
            arrive(ref, agz.at[kind, s])
        if k == 0:
            send(ref, ref, agz.at[kind, s], far)
        if k == 1:
            send(ref, ref, agz.at[kind, s], far, inner)
        else:
            send(ref, ref, agz.at[kind, s], near, inner)
        send(ref, ref, agx.at[kind, s], xn)
        if kind == 1:
            send(ref, ref, agy.at[kind, s], yn)
            ref = gath.at[blk(s, 0), A]
            send(ref, ref, agy.at[0, s], yn)

    def across(k):
        s = order[k]
        ref = gath.at[blk(s, sx), A]
        arrive(ref, agx.at[0, s])
        send(ref, ref, agd.at[0, s], yn)
        ref = gath.at[blk(s, sy), B]
        arrive(ref, agy.at[1, s])
        send(ref, ref, agd.at[1, s], xn)

    tile = tile_of(2 * ff, 256)

    def first_dots(k):
        s = order[k]
        arrive(gath.at[blk(s, sx), B], agx.at[1, s])
        arrive(gath.at[blk(s, sy), A], agy.at[0, s])
        arrive(gath.at[blk(s, sx + sy), A], agd.at[0, s])
        arrive(gath.at[blk(s, sx + sy), B], agd.at[1, s])
        if k == 0:
            loads[0].wait()
            loads[1].wait()
        at = pl.ds(pl.multiple_of(s * group, group), group)

        @pl.loop(0, 2 * ff // tile)
        def _(i):
            cols = pl.ds(pl.multiple_of(i * tile, tile), tile)
            gu[:, cols] = jnp.dot(gath[at, :], w1[:, cols], preferred_element_type=jnp.float32)

        gate, up = gu[:, :ff], gu[:, ff:]
        hid[at, :] = (jax.nn.gelu(gate, approximate=True) * up).astype(jnp.bfloat16)

    along(0,0)
    along(0,1)
    along(1,0)
    across(0)
    along(1,1)
    along(2,0)
    across(1)
    along(2,1)
    first_dots(0)
    along(3,0)
    across(2)
    along(3,1)
    first_dots(1)
    across(3)
    first_dots(2)
    first_dots(3)
    back = order[::-1]
    wide = tile_of(half, 768)

    def last_dot(j):
        s = back[j]
        if j == 0:
            loads[2].wait()
        at = pl.ds(pl.multiple_of(s * group, group), group)

        @pl.loop(0, d // wide)
        def _(i):
            cols = pl.ds(pl.multiple_of(i * wide, wide), wide)
            res = jnp.dot(hid[at, :], w2[:, cols], preferred_element_type=jnp.float32)
            part[at, cols] = res
            sendb[at, cols] = res.astype(jnp.bfloat16)

        send(sendb.at[blk(s, sx + sy), A], rda.at[s], rsd.at[0, s], xn)
        send(sendb.at[blk(s, sx + sy), B], rdb.at[s], rsd.at[1, s], yn)
        send(sendb.at[blk(s, sx), A], xr.at[s, :, A], rsx.at[0, s], xn)
        send(sendb.at[blk(s, sy), B], yr.at[s, :, B], rsy.at[1, s], yn)

    def pass_on(j):
        s = back[j]
        arrive(rda.at[s], rsd.at[0, s])
        at = blk(s, sy)
        sendb[at, A] = (part[at, A] + rda[s].astype(jnp.float32)).astype(jnp.bfloat16)
        send(sendb.at[at, A], yr.at[s, :, A], rsy.at[0, s], yn)
        arrive(rdb.at[s], rsd.at[1, s])
        at = blk(s, sx)
        sendb[at, B] = (part[at, B] + rdb[s].astype(jnp.float32)).astype(jnp.bfloat16)
        send(sendb.at[at, B], xr.at[s, :, B], rsx.at[1, s], xn)

    def settle(j):
        s = back[j]
        arrive(xr.at[s, :, A], rsx.at[0, s])
        arrive(yr.at[s, :, B], rsy.at[1, s])
        at = blk(s, 0)
        for kind, cols in enumerate(halves):
            if kind == 0:
                arrive(yr.at[s, :, A], rsy.at[0, s])
            else:
                arrive(xr.at[s, :, B], rsx.at[1, s])
            total = part[at, cols] + xr[s, :, cols].astype(jnp.float32) + yr[s, :, cols].astype(jnp.float32)
            part[at, cols] = total
            if j < LINE - 1:
                pl.when(outer)(functools.partial(ship, j, kind, far, flip, outer))

    def ship(j, kind, target, way, cond):
        s = back[j]
        at = blk(s, 0)
        sendb[at, halves[kind]] = part[at, halves[kind]].astype(jnp.bfloat16)
        send(sendb.at[at, halves[kind]], zr.at[way, s, :, halves[kind]], rsz.at[way, kind, s], target, cond, True)

    def add(j, way, kind):
        s = back[j]
        at = blk(s, 0)
        arrive(zr.at[way, s, :, halves[kind]], rsz.at[way, kind, s])
        part[at, halves[kind]] += zr[way, s, :, halves[kind]].astype(jnp.float32)

    outward, inward = flip, 1 - flip

    def follow(j):
        @pl.when(inner)
        def _():
            for kind in (0, 1):
                if j == LINE - 2:
                    add(j, inward, kind)
                    ship(j, kind, near, inward, inner)
                else:
                    add(j, outward, kind)
                    ship(j, kind, far, outward, inner)

    last_dot(0)
    last_dot(1)
    pass_on(0)
    last_dot(2)
    pass_on(1)
    last_dot(3)
    settle(0)
    pass_on(2)
    follow(0)
    settle(1)
    pass_on(3)
    follow(1)
    settle(2)
    follow(2)
    settle(3)
    for kind in (0, 1):
        add(LINE - 1, inward, kind)
        pl.when(inner)(functools.partial(add, LINE - 1, outward, kind))

    total = part[blk(z, 0), :]
    factor = lax.rsqrt(jnp.mean(total * total, axis=1, keepdims=True) + norm_eps)
    post = (total * factor * post_ref[...][None]).astype(jnp.bfloat16)
    stream = stream_ref[...].astype(jnp.float32)
    out_ref[...] = (stream + post.astype(jnp.float32)).astype(jnp.bfloat16)

    sent = sendb.at[pl.ds(0, rows), A]

    def drain(i):
        pltpu.make_async_remote_copy(
            src_ref=sent, dst_ref=sent, send_sem=ssem.at[i], recv_sem=rsd.at[0, 0],
            device_id={"tensor": xn}, device_id_type=MESH,
        ).wait_send()

    for i, cond in enumerate(pending):
        if cond is None:
            drain(i)
        else:
            pl.when(cond)(functools.partial(drain, i))


def fused(resid_stream, pre_gain, w_gate, w_up, w_down, post_gain):
    rows, d = resid_stream.shape
    ff = w_gate.shape[1]
    n = PLANE * LINE
    bf, f32, dma = jnp.bfloat16, jnp.float32, pltpu.SemaphoreType.DMA
    vmem = pl.BlockSpec(memory_space=pltpu.VMEM)
    hbm = pl.BlockSpec(memory_space=pl.ANY)
    return pl.pallas_call(
        kernel,
        out_shape=jax.ShapeDtypeStruct((rows, d), bf),
        in_specs=[vmem, vmem, hbm, hbm, hbm, vmem],
        out_specs=vmem,
        scratch_shapes=[
            pltpu.VMEM((d, 2 * ff), bf),
            pltpu.VMEM((ff, d), bf),
            pltpu.VMEM((n * rows, d), bf),
            pltpu.VMEM((PLANE * rows, 2 * ff), f32),
            pltpu.VMEM((n * rows, ff), bf),
            pltpu.VMEM((n * rows, d), f32),
            pltpu.VMEM((n * rows, d), bf),
            pltpu.VMEM((LINE, rows, d // 2), bf),
            pltpu.VMEM((LINE, rows, d // 2), bf),
            pltpu.VMEM((LINE, rows, d), bf),
            pltpu.VMEM((LINE, rows, d), bf),
            pltpu.VMEM((2, LINE, rows, d), bf),
            dma((3,)),
            dma((112,)),
            dma((2, LINE)),
            dma((2, LINE)),
            dma((2, LINE)),
            dma((2, LINE)),
            dma((2, LINE)),
            dma((2, LINE)),
            dma((2, LINE)),
            dma((2, 2, LINE)),
        ],
        compiler_params=pltpu.CompilerParams(
            collective_id=0, has_side_effects=True, vmem_limit_bytes=60 * 2**20
        ),
        name="ffn",
    )(resid_stream, pre_gain, w_gate, w_up, w_down, post_gain)


def solution(mesh):
    body = fused if mesh.shape["tensor"] == PLANE * LINE else shards
    return jax.shard_map(
        body,
        mesh=mesh,
        in_specs=(
            P(("dp", "tensor"), None),
            P(),
            P(None, "tensor"),
            P(None, "tensor"),
            P("tensor", None),
            P(),
        ),
        out_specs=P(("dp", "tensor"), None),
        check_vma=False,
    )
```

```python
import functools

import jax
import jax.numpy as jnp
from jax import lax
from jax.experimental import pallas as pl
from jax.experimental.pallas import tpu as pltpu
from jax.sharding import PartitionSpec as P

norm_eps = 1e-06
SIDE = 2
PLANE = SIDE * SIDE
TURNED = 4
LINE = 4
MESH = pl.DeviceIdType.MESH


def shards(resid_stream, pre_gain, w_gate, w_up, w_down, post_gain):
    stream = resid_stream.astype(jnp.float32)
    local_norm = stream * lax.rsqrt(jnp.mean(stream * stream, axis=1, keepdims=True) + norm_eps)
    normed = (local_norm * pre_gain).astype(jnp.bfloat16)
    row_piece = lax.all_gather(normed, "tensor", axis=0, tiled=True)
    gate_out = jnp.dot(row_piece, w_gate, preferred_element_type=jnp.float32)
    up_out = jnp.dot(row_piece, w_up, preferred_element_type=jnp.float32)
    hidden = (jax.nn.gelu(gate_out, approximate=True) * up_out).astype(jnp.bfloat16)
    block_rows = lax.psum_scatter(
        jnp.dot(hidden, w_down, preferred_element_type=jnp.float32),
        "tensor",
        scatter_dimension=0,
        tiled=True,
    )
    row_factor = lax.rsqrt(jnp.mean(block_rows * block_rows, axis=1, keepdims=True) + norm_eps)
    post = (block_rows * row_factor * post_gain).astype(jnp.bfloat16)
    post = lax.optimization_barrier(post)
    return (stream + post.astype(jnp.float32)).astype(jnp.bfloat16)


def tile_of(size, most):
    return max(t for t in range(128, most + 1, 128) if size % t == 0)


def cut(d):
    lanes = d // 128
    most = 2 * (TURNED * lanes // 36) + lanes % 2
    return (lanes - most) // 2 * 128, most * 128


def kernel(
    stream_ref, pre_ref, wg_hbm, wu_hbm, wd_hbm, post_ref, out_ref,
    w1, w2, gath, gu, hid, part, sendb, rda, rdb, xr, yr, zr,
    zrc, xyc,
    wsem, ssem, agz, agx, agy, agd, rsd, rsx, rsy, rsz, agp, agc, rsc, rsp,
):
    rows, d = stream_ref.shape
    ff = wg_hbm.shape[1]
    half, cw = cut(d)
    group = PLANE * rows
    A, B = halves = pl.ds(0, half), pl.ds(half, half)
    C = pl.ds(2 * half, cw)

    me = lax.axis_index("tensor")
    x = lax.rem(me, SIDE)
    y = lax.rem(lax.div(me, SIDE), SIDE)
    z = lax.div(me, PLANE)
    spot = lax.rem(me, PLANE)
    sx = 1 - 2 * x
    sy = SIDE * (1 - 2 * y)
    xn, yn, dn = me + sx, me + sy, me + sx + sy
    flip = lax.div(z, LINE // 2)
    p = z + flip * (LINE - 1 - 2 * z)
    inner, outer = p == 1, p == 0
    far = me + PLANE * (1 - 2 * flip)
    near = me - PLANE * (1 - 2 * flip)

    barrier = pltpu.get_barrier_semaphore()
    for other in (xn, yn, dn, far):
        pl.semaphore_signal(barrier, inc=1, device_id={"tensor": other}, device_id_type=MESH)

    @pl.when(inner)
    def _():
        pl.semaphore_signal(barrier, inc=1, device_id={"tensor": near}, device_id_type=MESH)

    loads = [
        pltpu.make_async_copy(wg_hbm, w1.at[:, pl.ds(0, ff)], wsem.at[0]),
        pltpu.make_async_copy(wu_hbm, w1.at[:, pl.ds(ff, ff)], wsem.at[1]),
        pltpu.make_async_copy(wd_hbm, w2, wsem.at[2]),
    ]
    for load in loads:
        load.start()

    def plane_of(v):
        return v + flip * (LINE - 1 - 2 * v)

    order = [plane_of(p), plane_of(1 - p), plane_of(2), plane_of(3)]

    def blk(s, shift):
        return pl.ds(pl.multiple_of((s * PLANE + spot + shift) * rows, rows), rows)

    pending = []

    def send(src, dst, recv_sem, target, cond=None, inside=False):
        copy = pltpu.make_async_remote_copy(
            src_ref=src, dst_ref=dst, send_sem=ssem.at[len(pending)], recv_sem=recv_sem,
            device_id={"tensor": target}, device_id_type=MESH,
        )
        pending.append((cond, src.shape))
        if cond is None or inside:
            copy.start()
        else:
            pl.when(cond)(copy.start)

    def arrive(dst, recv_sem):
        pltpu.make_async_remote_copy(
            src_ref=dst, dst_ref=dst, send_sem=ssem.at[0], recv_sem=recv_sem,
            device_id={"tensor": xn}, device_id_type=MESH,
        ).wait_recv()

    stream = stream_ref[...].astype(jnp.float32)
    scale = lax.rsqrt(jnp.mean(stream * stream, axis=1, keepdims=True) + norm_eps)
    gath[blk(z, 0), :] = (stream * scale * pre_ref[...][None]).astype(jnp.bfloat16)

    pl.semaphore_wait(barrier, 4 + p)

    def along(k, kind):
        s = order[k]
        ref = gath.at[blk(s, 0), halves[kind]]
        if k > 0:
            arrive(ref, agz.at[kind, s])
        if k == 0:
            send(ref, ref, agz.at[kind, s], far)
        if k == 1:
            send(ref, ref, agz.at[kind, s], far, inner)
        else:
            send(ref, ref, agz.at[kind, s], near, inner)
        send(ref, ref, agx.at[kind, s], xn)
        if kind == 1:
            send(ref, ref, agy.at[kind, s], yn)
            ref = gath.at[blk(s, 0), A]
            send(ref, ref, agy.at[0, s], yn)

    def across(k):
        s = order[k]
        ref = gath.at[blk(s, sx), A]
        arrive(ref, agx.at[0, s])
        send(ref, ref, agd.at[0, s], yn)
        ref = gath.at[blk(s, sy), B]
        arrive(ref, agy.at[1, s])
        send(ref, ref, agd.at[1, s], xn)

    around = ((sx, xn), (sy, yn), (sx + sy, dn))

    def plane(s):
        return pl.ds(pl.multiple_of(s * group, group), group)

    def spread():
        ref = gath.at[blk(z, 0), C]
        for i, (_, other) in enumerate(around):
            send(ref, ref, agp.at[i], other)

    def relay(k):
        s = order[k]
        ref = gath.at[plane(s), C]
        if k == 0:
            for i, (shift, _) in enumerate(around):
                arrive(gath.at[blk(s, shift), C], agp.at[i])
            send(ref, ref, agc.at[s], far)
        else:
            arrive(ref, agc.at[s])
        if k == 1:
            send(ref, ref, agc.at[s], far, inner)
        else:
            send(ref, ref, agc.at[s], near, inner)

    tile = tile_of(2 * ff, 256)

    def first_dots(k):
        s = order[k]
        arrive(gath.at[blk(s, sx), B], agx.at[1, s])
        arrive(gath.at[blk(s, sy), A], agy.at[0, s])
        arrive(gath.at[blk(s, sx + sy), A], agd.at[0, s])
        arrive(gath.at[blk(s, sx + sy), B], agd.at[1, s])
        if k == 0:
            loads[0].wait()
            loads[1].wait()
        at = pl.ds(pl.multiple_of(s * group, group), group)

        @pl.loop(0, 2 * ff // tile)
        def _(i):
            cols = pl.ds(pl.multiple_of(i * tile, tile), tile)
            gu[:, cols] = jnp.dot(gath[at, :], w1[:, cols], preferred_element_type=jnp.float32)

        gate, up = gu[:, :ff], gu[:, ff:]
        hid[at, :] = (jax.nn.gelu(gate, approximate=True) * up).astype(jnp.bfloat16)

    spread()
    along(0, 0)
    along(0, 1)
    along(1, 0)
    across(0)
    along(1, 1)
    relay(0)
    along(2, 0)
    across(1)
    along(2, 1)
    first_dots(0)
    along(3, 0)
    across(2)
    along(3, 1)
    relay(1)
    relay(2)
    across(3)
    first_dots(1)
    relay(3)
    first_dots(2)
    first_dots(3)

    back = order[::-1]
    wide = tile_of(d, 768)

    def last_dot(j):
        s = back[j]
        if j == 0:
            loads[2].wait()
        at = pl.ds(pl.multiple_of(s * group, group), group)

        @pl.loop(0, d // wide)
        def _(i):
            cols = pl.ds(pl.multiple_of(i * wide, wide), wide)
            res = jnp.dot(hid[at, :], w2[:, cols], preferred_element_type=jnp.float32)
            part[at, cols] = res
            sendb[at, cols] = res.astype(jnp.bfloat16)

        send(sendb.at[blk(s, sx + sy), A], rda.at[s], rsd.at[0, s], xn)
        send(sendb.at[blk(s, sx + sy), B], rdb.at[s], rsd.at[1, s], yn)
        send(sendb.at[blk(s, sx), A], xr.at[s, :, A], rsx.at[0, s], xn)
        send(sendb.at[blk(s, sy), B], yr.at[s, :, B], rsy.at[1, s], yn)

    def pass_on(j):
        s = back[j]
        arrive(rda.at[s], rsd.at[0, s])
        at = blk(s, sy)
        sendb[at, A] = (part[at, A] + rda[s].astype(jnp.float32)).astype(jnp.bfloat16)
        send(sendb.at[at, A], yr.at[s, :, A], rsy.at[0, s], yn)
        arrive(rdb.at[s], rsd.at[1, s])
        at = blk(s, sx)
        sendb[at, B] = (part[at, B] + rdb[s].astype(jnp.float32)).astype(jnp.bfloat16)
        send(sendb.at[at, B], xr.at[s, :, B], rsx.at[1, s], xn)

    def settle(j):
        s = back[j]
        arrive(xr.at[s, :, A], rsx.at[0, s])
        arrive(yr.at[s, :, B], rsy.at[1, s])
        at = blk(s, 0)
        for kind, cols in enumerate(halves):
            if kind == 0:
                arrive(yr.at[s, :, A], rsy.at[0, s])
            else:
                arrive(xr.at[s, :, B], rsx.at[1, s])
            total = part[at, cols] + xr[s, :, cols].astype(jnp.float32) + yr[s, :, cols].astype(jnp.float32)
            part[at, cols] = total
            if j < LINE - 1:
                pl.when(outer)(functools.partial(ship, j, kind, far, flip, outer))

    def ship(j, kind, target, way, cond):
        s = back[j]
        at = blk(s, 0)
        sendb[at, halves[kind]] = part[at, halves[kind]].astype(jnp.bfloat16)
        send(sendb.at[at, halves[kind]], zr.at[way, s, :, halves[kind]], rsz.at[way, kind, s], target, cond, True)

    def add(j, way, kind):
        s = back[j]
        at = blk(s, 0)
        arrive(zr.at[way, s, :, halves[kind]], rsz.at[way, kind, s])
        part[at, halves[kind]] += zr[way, s, :, halves[kind]].astype(jnp.float32)

    outward, inward = flip, 1 - flip

    def follow(j):
        @pl.when(inner)
        def _():
            for kind in (0, 1):
                if j == LINE - 2:
                    add(j, inward, kind)
                    ship(j, kind, near, inward, inner)
                else:
                    add(j, outward, kind)
                    ship(j, kind, far, outward, inner)

    def turn(j):
        s = back[j]
        send(sendb.at[plane(s), C], zrc.at[flip, s], rsc.at[flip, s], far, outer)

    def add_turned(s, way):
        arrive(zrc.at[way, s], rsc.at[way, s])
        part[plane(s), C] += zrc[way, s].astype(jnp.float32)

    def turn_on(j):
        @pl.when(inner)
        def _():
            s = back[j]
            way, target = (inward, near) if j == LINE - 2 else (outward, far)
            add_turned(s, way)
            sendb[plane(s), C] = part[plane(s), C].astype(jnp.bfloat16)
            send(sendb.at[plane(s), C], zrc.at[way, s], rsc.at[way, s], target, inner, True)

    def share():
        s = back[LINE - 1]
        add_turned(s, inward)
        pl.when(inner)(lambda: add_turned(back[LINE - 1], outward))
        sendb[plane(s), C] = part[plane(s), C].astype(jnp.bfloat16)
        for i, (shift, other) in enumerate(around):
            send(sendb.at[blk(s, shift), C], xyc.at[i], rsp.at[i], other)

    def gain():
        for i in range(len(around)):
            arrive(xyc.at[i], rsp.at[i])
        at = blk(z, 0)
        part[at, C] += xyc[0].astype(jnp.float32) + xyc[1].astype(jnp.float32) + xyc[2].astype(jnp.float32)

    def close():
        for kind in (0, 1):
            add(LINE - 1, inward, kind)
            pl.when(inner)(functools.partial(add, LINE - 1, outward, kind))

    last_dot(0)
    turn(0)
    last_dot(1)
    turn(1)
    pass_on(0)
    last_dot(2)
    turn(2)
    pass_on(1)
    turn_on(0)
    last_dot(3)
    settle(0)
    turn_on(1)
    pass_on(2)
    follow(0)
    turn_on(2)
    settle(1)
    pass_on(3)
    follow(1)
    settle(2)
    share()
    follow(2)
    settle(3)
    close()
    gain()

    total = part[blk(z, 0), :]
    factor = lax.rsqrt(jnp.mean(total * total, axis=1, keepdims=True) + norm_eps)
    post = (total * factor * post_ref[...][None]).astype(jnp.bfloat16)
    stream = stream_ref[...].astype(jnp.float32)
    out_ref[...] = (stream + post.astype(jnp.float32)).astype(jnp.bfloat16)

    def drain(i, size):
        sent = sendb.at[pl.ds(0, size[0]), pl.ds(0, size[1])]
        pltpu.make_async_remote_copy(
            src_ref=sent, dst_ref=sent, send_sem=ssem.at[i], recv_sem=rsd.at[0, 0],
            device_id={"tensor": xn}, device_id_type=MESH,
        ).wait_send()

    for i, (cond, size) in enumerate(pending):
        if cond is None:
            drain(i, size)
        else:
            pl.when(cond)(functools.partial(drain, i, size))


def fused(resid_stream, pre_gain, w_gate, w_up, w_down, post_gain):
    rows, d = resid_stream.shape
    ff = w_gate.shape[1]
    half, cw = cut(d)
    n = PLANE * LINE
    bf, f32, dma = jnp.bfloat16, jnp.float32, pltpu.SemaphoreType.DMA
    vmem = pl.BlockSpec(memory_space=pltpu.VMEM)
    hbm = pl.BlockSpec(memory_space=pl.ANY)
    return pl.pallas_call(
        kernel,
        out_shape=jax.ShapeDtypeStruct((rows, d), bf),
        in_specs=[vmem, vmem, hbm, hbm, hbm, vmem],
        out_specs=vmem,
        scratch_shapes=[
            pltpu.VMEM((d, 2 * ff), bf),
            pltpu.VMEM((ff, d), bf),
            pltpu.VMEM((n * rows, d), bf),
            pltpu.VMEM((PLANE * rows, 2 * ff), f32),
            pltpu.VMEM((n * rows, ff), bf),
            pltpu.VMEM((n * rows, d), f32),
            pltpu.VMEM((n * rows, d), bf),
            pltpu.VMEM((LINE, rows, half), bf),
            pltpu.VMEM((LINE, rows, half), bf),
            pltpu.VMEM((LINE, rows, d), bf),
            pltpu.VMEM((LINE, rows, d), bf),
            pltpu.VMEM((2, LINE, rows, d), bf),
            pltpu.VMEM((2, LINE, PLANE * rows, cw), bf),
            pltpu.VMEM((3, rows, cw), bf),
            dma((3,)),
            dma((144,)),
            dma((2, LINE)),
            dma((2, LINE)),
            dma((2, LINE)),
            dma((2, LINE)),
            dma((2, LINE)),
            dma((2, LINE)),
            dma((2, LINE)),
            dma((2, 2, LINE)),
            dma((3,)),
            dma((LINE,)),
            dma((2, LINE)),
            dma((3,)),
        ],
        compiler_params=pltpu.CompilerParams(
            collective_id=0, has_side_effects=True, vmem_limit_bytes=60 * 2**20
        ),
        name="ffn",
    )(resid_stream, pre_gain, w_gate, w_up, w_down, post_gain)


def solution(mesh):
    body = fused if mesh.shape["tensor"] == PLANE * LINE else shards
    return jax.shard_map(
        body,
        mesh=mesh,
        in_specs=(
            P(("dp", "tensor"), None),
            P(),
            P(None, "tensor"),
            P(None, "tensor"),
            P("tensor", None),
            P(),
        ),
        out_specs=P(("dp", "tensor"), None),
        check_vma=False,
    )
```
